128 devices in a mesh: dp: 32 (over x, z, core), expert: 4 (over y).
Axes of the slice: x: 4, y: 4, z: 4, core: 2. Of those that a mesh axis runs over, the one named last changes fastest.
Arguments:
- tokens: bfloat16 [8192, 2048], P('dp'), may hold values from -6 to 6
- routes: int32 [8192, 6], P('dp'), may hold values from 0 to 63, all different within a row; in each aligned block of 256 rows (0 to 255, 256 to 511, ...) at most 32 rows name the same one
- gates: float32 [8192, 6], P('dp'), may hold values from 0.1 to 1
- w_gate: bfloat16 [64, 2048, 1408], P('dp', None, 'expert'), may hold values from -0.125 to 0.125
- w_up: bfloat16 [64, 2048, 1408], P('dp', None, 'expert'), may hold values from -0.125 to 0.125
- w_down: bfloat16 [64, 1408, 2048], P('dp', 'expert'), may hold values from -0.21875 to 0.21875
- s_gate: bfloat16 [2048, 2816], P(None, 'expert'), may hold values from -0.125 to 0.125
- s_up: bfloat16 [2048, 2816], P(None, 'expert'), may hold values from -0.125 to 0.125
- s_down: bfloat16 [2816, 2048], P('expert'), may hold values from -0.15625 to 0.15625
Outputs:
- mixed: bfloat16 [8192, 2048], P('dp', 'expert')
The draws below stay inside these ranges and needn't reach their ends.
Inputs may be any that keep to these rules, and one draw needn't show every extreme that they name: `routes`: each row names 6 different experts. Within each aligned block of 256 rows (the rows of one index of dp) no expert is named by more than 32 rows; some expert is named by exactly 32 rows in some block of every draw.
All inputs are finite; a program needn't handle non-finite values.
Results may differ from the reference program's by a relative error of at most 0.013.
Values may be sent and summed in bfloat16 or wider, within the bound.
A program may use at most 128 MiB of HBM per device.

```python
import math
import jax
import jax.numpy as jnp
import numpy as np
from jax import lax

D = 2048
FF = 1408
SFF = 2816
EXPERTS = 64
TOP = 6
TOK_DEV = 256
CAP = 32
TOKENS = 8192
N_DP = 32
N_EXPERT = 4


def strengthened(values, own_key, source, target, shards_of, factor):
    def block_of(axis_at):
        return (jnp.arange(values.shape[axis_at]) // (values.shape[axis_at] // shards_of)).reshape((-1,) + (1,) * (values.ndim - 1 - axis_at))

    near = jax.random.permutation(own_key, shards_of)[block_of(target)]
    second = (block_of(target) + shards_of // 2) % shards_of
    return jnp.where((block_of(source) == near) | (block_of(source) == second), factor * values, values)


def level_of(rng, extent, shards, least, largest):
    def one(axis_at, blocks):
        steps = jax.random.uniform(jax.random.fold_in(jax.random.fold_in(rng, 6), axis_at), (blocks,), jnp.float32, least / len(shards), largest / len(shards))
        return jnp.repeat(jnp.exp(steps), extent[axis_at] // blocks).reshape((-1,) + (1,) * (len(extent) - axis_at - 1))

    gain = one(*shards[0])
    for cut in shards[1:]:
        gain = gain * one(*cut)
    return gain


def assign_block(rng, own, number, rows, amount, top, reach, lean):
    ranking = jax.random.permutation(rng, amount)
    heavy_load, common = shares(amount, rows * top, reach, lean, True), shares(amount, rows * top, reach, lean, False)
    places = jnp.arange(amount)

    def named(sizes, turn):
        used = int((sizes > 0).sum())
        fixed = max(1, used // 4)
        moved = fixed + (places - fixed + turn * (used - fixed)) % max(1, amount - fixed)
        return jnp.zeros((amount,), jnp.int32).at[ranking[jnp.where(places < fixed, places, moved)]].set(jnp.asarray(sizes, jnp.int32))

    sizes = jnp.where(number % 4 == 0, named(heavy_load, number // 4), named(common, number - number // 4 - 1))
    mixed = jax.random.permutation(jax.random.fold_in(own, 3), amount)
    donor, taker = mixed[0:amount // 2 * 2:2], mixed[1:amount // 2 * 2:2]
    room = jnp.minimum(sizes[donor] - 1, reach - sizes[taker]) // 2
    room = jnp.where((donor == ranking[0]) | (taker == ranking[0]) | (sizes[taker] == 0), 0, jnp.maximum(room, 0))
    moved = jax.random.randint(jax.random.fold_in(own, 4), (amount // 2,), 0, 1 << 20) % (room + 1)
    sizes = sizes.at[donor].add(-moved).at[taker].add(moved)
    members = jnp.searchsorted(jnp.cumsum(sizes), jnp.arange(rows * top), side="right").astype(jnp.int32)
    grid = members.reshape(top, rows).T
    grid = grid[jax.random.permutation(jax.random.fold_in(own, 1), rows)]
    turn = jax.random.randint(jax.random.fold_in(own, 2), (rows, 1), 0, top)
    return jnp.take_along_axis(grid, (jnp.arange(top)[None, :] + turn) % top, axis=1)


def shares(amount, total, most, skew, full):
    weights = [(1 << 20) // math.isqrt(standing ** skew) + 1 for standing in range(1, amount + 1)]
    largest = most if full else min(most, max(-(-total // amount), total * weights[0] // sum(weights)))
    least = 1 if total - largest >= amount - 1 else 0
    given, spare = [largest] + [least] * (amount - 1), total - largest - least * (amount - 1)
    while spare > 0:
        candidates = [i for i in range(1, amount) if given[i] < largest] or [i for i in range(1, amount) if given[i] < most]
        mass, left = sum([weights[i] for i in candidates]), spare
        for i in candidates:
            more = min(most - given[i], max(1, left * weights[i] // mass), spare)
            given[i] = given[i] + more
            spare = spare - more
    return np.array(given)


def noise(rng, extent, deviation, reach, split=(), kind=jnp.bfloat16):
    gain = level_of(rng, extent, split, -0.22, 0.18) if split else 1.0
    array = jax.random.normal(rng, extent, jnp.float32) * deviation * gain
    return jnp.minimum(jnp.maximum(array, -reach), reach).astype(kind)


def bell_draw_with(own_key, dims, spread, bound, split, heavy, kind=jnp.bfloat16):
    result = spread * jax.random.normal(own_key, dims, jnp.float32)
    if split:
        result = result * level_of(own_key, dims, split, -0.22, 0.18)
    return jnp.clip(strengthened(result, jax.random.fold_in(own_key, 3), *heavy), -bound, bound).astype(kind)


def setup_inputs(seed: int = 0) -> dict:
    splits = jax.random.split(jax.random.key(seed), 10)
    tokens = noise(splits[0], (TOKENS, D), 1.0, 6.0, ((0, 32),))
    routes_keys = jax.random.split(jax.random.fold_in(splits[1], 1), TOKENS // TOK_DEV)
    routes_turns = jax.random.permutation(jax.random.fold_in(splits[1], 3), TOKENS // TOK_DEV)
    routes = jax.vmap(lambda own, number: assign_block(jax.random.fold_in(splits[1], 2), own, number, TOK_DEV, EXPERTS, TOP, CAP, 2))(routes_keys, routes_turns).reshape((TOKENS, TOP))
    gates = jnp.clip(jnp.exp(math.log(1.0) - 2.3025851 * jax.random.uniform(splits[2], (TOKENS, TOP), jnp.float32) ** level_of(splits[2], (TOKENS, TOP), ((0, 32),), -0.2, 0.2)), 0.1, 1.0)
    w_gate = noise(splits[3], (EXPERTS, D, FF), D ** -0.5, 0.125, ((0, 32), (2, 4)))
    w_up = noise(splits[4], (EXPERTS, D, FF), D ** -0.5, 0.125, ((0, 32), (2, 4)))
    w_down = bell_draw_with(splits[5], (EXPERTS, FF, D), FF ** -0.5, 0.21875, ((0, 32), (1, 4)), (1, 2, 4, 2.0))
    s_gate = noise(splits[6], (D, SFF), D ** -0.5, 0.125, ((1, 4),))
    s_up = noise(splits[7], (D, SFF), D ** -0.5, 0.125, ((1, 4),))
    s_down = bell_draw_with(splits[8], (SFF, D), SFF ** -0.5, 0.15625, ((0, 4),), (0, 1, 4, 2.0))
    return {"tokens": tokens, "routes": routes, "gates": gates, "w_gate": w_gate, "w_up": w_up, "w_down": w_down, "s_gate": s_gate, "s_up": s_up, "s_down": s_down}


def quarter_sum(hidden, down, parts):
    inner = hidden.shape[1] // parts
    partial_value = jnp.einsum("rqf,qfd->rqd", hidden.reshape(hidden.shape[0], parts, inner).astype(jnp.float32), down.reshape(parts, inner, down.shape[1]).astype(jnp.float32))
    rounded = lax.optimization_barrier(partial_value.astype(jnp.bfloat16))
    return jnp.sum(rounded.astype(jnp.float32), axis=1)


def reference(tokens, routes, gates, w_gate, w_up, w_down, s_gate, s_up, s_down):
    blocks = routes.reshape(N_DP, TOK_DEV, TOP)
    labels = jnp.arange(EXPERTS, dtype=jnp.int32)
    matches = (blocks[:, :, :, None] == labels[None, None, None, :]).astype(jnp.int32)
    counts = jnp.sum(matches, axis=2).astype(jnp.int32)
    before = (jnp.cumsum(counts, axis=1) - counts).astype(jnp.int32)
    slots = jnp.sum(matches * before[:, :, None, :], axis=3).astype(jnp.int32)
    owner_block = jnp.arange(N_DP, dtype=jnp.int32)[:, None, None]
    dest = ((blocks * N_DP + owner_block) * CAP + slots).astype(jnp.int32)
    token_ids = owner_block * TOK_DEV + jnp.arange(TOK_DEV, dtype=jnp.int32)[None, :, None] + jnp.zeros((1, 1, TOP), jnp.int32)
    sources = jnp.full((EXPERTS * N_DP * CAP,), TOKENS, jnp.int32).at[dest.reshape(-1)].set(token_ids.reshape(-1).astype(jnp.int32))
    padded = jnp.concatenate([tokens, jnp.zeros((1, D), tokens.dtype)], axis=0)

    def one_expert(inputs):
        table, gate_w, up_w, down_w = inputs
        rows = padded[table]
        gate = jnp.dot(rows, gate_w, preferred_element_type=jnp.float32)
        up = jnp.dot(rows, up_w, preferred_element_type=jnp.float32)
        hidden = (jax.nn.silu(gate) * up).astype(jnp.bfloat16)
        return quarter_sum(hidden, down_w, N_EXPERT).astype(jnp.bfloat16)

    outputs = lax.map(one_expert, (sources.reshape(EXPERTS, N_DP * CAP), w_gate, w_up, w_down))
    flat = outputs.reshape(EXPERTS * N_DP * CAP, D)
    picked = flat[dest.reshape(TOKENS, TOP)].astype(jnp.float32)
    routed = jnp.einsum("tk,tkd->td", gates.astype(jnp.float32), picked)
    shared_gate = jnp.dot(tokens, s_gate, preferred_element_type=jnp.float32)
    shared_up = jnp.dot(tokens, s_up, preferred_element_type=jnp.float32)
    shared_hidden = (jax.nn.silu(shared_gate) * shared_up).astype(jnp.bfloat16)
    shared_out = quarter_sum(shared_hidden, s_down, N_EXPERT)
    return (shared_out + routed).astype(jnp.bfloat16)
```

```python
import jax
import jax.numpy as jnp
from jax import lax
from jax.experimental import pallas as pl
from jax.experimental.pallas import tpu as pltpu
from jax.sharding import PartitionSpec as P

MESH = pl.DeviceIdType.MESH
BF16 = jnp.bfloat16
F32 = jnp.float32
CAP = 32
CHUNK = 512
WHOLE = (0, 1)
SPLIT = (3, 2)


def dot(a, b):
    return jnp.dot(a, b, preferred_element_type=F32)


def silu(v):
    return v / (1.0 + jnp.exp(-v))


def kernel(
    tok, routes_t, gates_t, wg_h, wu_h, wd_h, sg_h, su_h, sd_h, out,
    info, xinfo, xbuf, slots, zst_a, zst_s, zst_b, ybuf, ysum, zr_a, zr_s, zr_b, xr, acc, y2s, y2r,
    pick, hid, shid, wg, wu, wd, sg, su, sd,
    sx, rx, si, ri, sz, rz, sy, ry, szr, rzr, syr, ryr, sxr, rxr, sy2, ry2, wsem,
):
    me = lax.axis_index("dp")
    y = lax.axis_index("expert")
    x = lax.div(me, 8)
    z = lax.rem(lax.div(me, 2), 4)
    c = lax.rem(me, 2)
    width = tok.shape[1]
    chunks = width // CHUNK

    def at_x(d):
        return {"dp": lax.rem(x + d + 4, 4) * 8 + z * 2 + c}

    def core_of(cc):
        return c if cc == 0 else 1 - c

    def at_z(d, cc):
        return {"dp": x * 8 + lax.rem(z + d + 4, 4) * 2 + core_of(cc)}

    def at_y(p):
        return {"expert": lax.rem(y + p, 4)}

    def remote(src, dst, s, r, where):
        return pltpu.make_async_remote_copy(
            src_ref=src, dst_ref=dst, send_sem=s, recv_sem=r, device_id=where, device_id_type=MESH
        )

    peers = [at_x(d) for d in (1, 2, 3)]
    peers += [at_z(r // 2, r % 2) for r in range(1, 8)]
    peers += [at_y(p) for p in (1, 2, 3)]
    barrier = pltpu.get_barrier_semaphore()
    for peer in peers:
        pl.semaphore_signal(barrier, inc=1, device_id=peer, device_id_type=MESH)
    loads = [
        pltpu.make_async_copy(src, dst, wsem.at[i])
        for i, (src, dst) in enumerate(
            ((sg_h, sg), (su_h, su), (sd_h, sd), (wg_h, wg), (wu_h, wu), (wd_h, wd))
        )
    ]
    for load in loads:
        load.start()
    pl.semaphore_wait(barrier, len(peers))

    near = {
        1: remote(tok, xbuf.at[0], sx.at[0], rx.at[0], at_x(-1)),
        3: remote(tok, xbuf.at[2], sx.at[1], rx.at[1], at_x(1)),
    }
    near[1].start()
    near[3].start()
    half = tok.shape[0] // 2
    relay = {
        1: remote(
            xbuf.at[0, pl.ds(0, half)], xbuf.at[1, pl.ds(0, half)], sx.at[2], rx.at[2], at_x(-1)
        ),
        3: remote(
            xbuf.at[2, pl.ds(half, half)], xbuf.at[1, pl.ds(half, half)], sx.at[3], rx.at[3], at_x(1)
        ),
    }

    rt = routes_t[...]
    rows = tok.shape[0]
    label = lax.broadcasted_iota(jnp.int32, (64, rows), 0)
    hits = jnp.zeros((64, rows), F32)
    for k in range(6):
        hits = hits + jnp.where(rt[k : k + 1, :] == label, 1.0, 0.0)
    earlier = jnp.where(
        lax.broadcasted_iota(jnp.int32, (rows, rows), 0)
        < lax.broadcasted_iota(jnp.int32, (rows, rows), 1),
        1.0,
        0.0,
    )
    before = dot(hits.astype(BF16), earlier.astype(BF16))
    info[...] = jnp.full(info.shape, -1.0, F32)
    for k in range(6):
        slot = jnp.sum(jnp.where(rt[k : k + 1, :] == label, before, 0.0), axis=0, keepdims=True)
        info[k : k + 1, :] = rt[k : k + 1, :].astype(F32) * CAP + slot
        info[8 + k : 9 + k, :] = gates_t[k : k + 1, :]
    tell = {
        j: remote(info, xinfo.at[j - 1], si.at[j - 1], ri.at[j - 1], at_x(-j)) for j in (1, 2, 3)
    }
    for j in (1, 3, 2):
        tell[j].start()

    def base_of(r):
        return (x * 8 + lax.rem(z + r // 2, 4) * 2 + core_of(r % 2)) * 64

    def select(table, base, count, at, weighted):
        ids = (lax.broadcasted_iota(jnp.int32, (count, rows), 0) + base).astype(F32)
        value = jnp.zeros((count, rows), F32)
        for k in range(6):
            given = table[8 + k : 9 + k, :] if weighted else 1.0
            value = value + jnp.where(ids == table[k : k + 1, :], given, 0.0)
        pick[at : at + count, :] = value.astype(BF16)

    def select_whole(table, weighted):
        for r in range(8):
            select(table, base_of(r), 64, r * 64, weighted)

    def select_split(table, weighted):
        for r in range(2):
            select(table, base_of(r), 64, r * 64, weighted)
        for r in range(2, 8):
            select(table, base_of(r) + 16 * y, 16, 128 + (r - 2) * 16, weighted)

    e_y, h_y = lax.div(y, 2), pl.multiple_of(lax.rem(y, 2) * 16, 16)

    zd = {}
    select_whole(info, False)

    @pl.loop(0, chunks)
    def _(i):
        cols = pl.ds(pl.multiple_of(i * CHUNK, CHUNK), CHUNK)
        packed = dot(pick[...], tok[:, cols]).astype(BF16)
        slots[0, :, 0, :, cols] = packed[:64].reshape(2, 32, CHUNK)
        zst_a[:, :, :, cols] = packed[64:].reshape(7, 2, 32, CHUNK)

    for r in (2, 6, 4, 3, 7, 5, 1):
        zd[0, r] = remote(
            zst_a.at[r - 1], slots.at[0, :, r], sz.at[0, r], rz.at[0, r], at_z(r // 2, r % 2)
        )
        zd[0, r].start()

    for load in loads[:3]:
        load.wait()
    gate = dot(tok[...], sg[...])
    up = dot(tok[...], su[...])
    shid[...] = (silu(gate) * up).astype(BF16)

    @pl.loop(0, chunks)
    def _(i):
        cols = pl.ds(pl.multiple_of(i * CHUNK, CHUNK), CHUNK)
        acc[:, cols] = dot(shid[...], sd[:, cols])

    def pack_split(j):
        select_split(xinfo.at[j - 1], False)

        @pl.loop(0, chunks)
        def _(i):
            cols = pl.ds(pl.multiple_of(i * CHUNK, CHUNK), CHUNK)
            packed = dot(pick[:224, :], xbuf[j - 1, :, cols]).astype(BF16)
            slots[j, :, 0, :, cols] = packed[:64].reshape(2, 32, CHUNK)
            zst_s[j - 1, :, :, cols] = packed[64:128].reshape(2, 32, CHUNK)
            zst_b[j - 1, :, :, cols] = packed[128:224].reshape(6, 16, CHUNK)

        for r in (2, 6, 4, 3, 7, 5):
            zd[j, r] = remote(
                zst_b.at[j - 1, r - 2],
                slots.at[j, e_y, r, pl.ds(h_y, 16)],
                sz.at[j, r],
                rz.at[j, r],
                at_z(r // 2, r % 2),
            )
            zd[j, r].start()
        zd[j, 1] = remote(
            zst_s.at[j - 1], slots.at[j, :, 1], sz.at[j, 1], rz.at[j, 1], at_z(0, 1)
        )
        zd[j, 1].start()

    yd = {}

    def forward(j):
        for r in (2, 6, 4, 3, 7, 5):
            zd[j, r].wait_recv()
        mine = slots.at[j, e_y, pl.ds(2, 6), pl.ds(h_y, 16)]
        for p in (1, 3, 2):
            yd[j, p] = remote(mine, mine, sy.at[j, p], ry.at[j, p], at_y(p))
            yd[j, p].start()

    back = {}
    yb = {}

    def experts(j):
        if j == 0:
            for load in loads[3:]:
                load.wait()
            for r in range(2, 8):
                zd[j, r].wait_recv()
        else:
            for p in (1, 3, 2):
                yd[j, p].wait_recv()
                yd[j, p].wait_send()
        zd[j, 1].wait_recv()

        @pl.loop(0, 2)
        def _(e):
            given = slots[j, e].reshape(256, width)
            gate = dot(given, wg[e])
            up = dot(given, wu[e])
            hid[...] = (silu(gate) * up).astype(BF16)

            @pl.loop(0, chunks)
            def _(i):
                cols = pl.ds(pl.multiple_of(i * CHUNK, CHUNK), CHUNK)
                slots[j, e, :, :, cols] = (
                    dot(hid[...], wd[e, :, cols]).astype(BF16).reshape(8, 32, CHUNK)
                )

        if j in WHOLE:
            for r in (2, 6, 4, 3, 7, 5, 1):
                back[j, r] = remote(
                    slots.at[j, :, r],
                    zr_a.at[j, r],
                    szr.at[j, r],
                    rzr.at[j, r],
                    at_z(-(r // 2), r % 2),
                )
                back[j, r].start()
            zr_a[j, 0] = slots[j, :, 0]
        else:
            n = SPLIT.index(j)
            for p in (1, 3, 2):
                to = lax.rem(y + p, 4)
                yb[j, p] = remote(
                    slots.at[
                        j, lax.div(to, 2), pl.ds(2, 6), pl.ds(pl.multiple_of(lax.rem(to, 2) * 16, 16), 16)
                    ],
                    ybuf.at[n, p - 1],
                    syr.at[j, p],
                    ryr.at[j, p],
                    at_y(p),
                )
                yb[j, p].start()
            back[j, 1] = remote(
                slots.at[j, :, 1], zr_s.at[n, 1], szr.at[j, 1], rzr.at[j, 1], at_z(0, 1)
            )
            back[j, 1].start()
            zr_s[n, 0] = slots[j, :, 0]

    def sum_over_y(j):
        n = SPLIT.index(j)
        for p in (1, 3, 2):
            yb[j, p].wait_recv()

        @pl.loop(0, chunks)
        def _(i):
            cols = pl.ds(pl.multiple_of(i * CHUNK, CHUNK), CHUNK)
            total = slots[j, e_y, 2:8, pl.ds(h_y, 16), cols].astype(F32)
            for p in range(3):
                total = total + ybuf[n, p, :, :, cols].astype(F32)
            ysum[n, :, :, cols] = total.astype(BF16)

        for r in (2, 6, 4, 3, 7, 5):
            back[j, r] = remote(
                ysum.at[n, r - 2],
                zr_b.at[n, r - 2],
                szr.at[j, r],
                rzr.at[j, r],
                at_z(-(r // 2), r % 2),
            )
            back[j, r].start()

    def weigh(a, b):
        return lax.dot_general(a, b, (((0,), (0,)), ((), ())), preferred_element_type=F32)

    xd = {}

    def combine(j):
        table = info if j == 0 else xinfo.at[j - 1]
        if j in WHOLE:
            select_whole(table, True)
        else:
            select_split(table, True)
        for r in range(1, 8):
            back[j, r].wait_recv()
        if j == 1:
            relay[1].wait_send()
        if j == 3:
            relay[3].wait_send()

        @pl.loop(0, chunks)
        def _(i):
            cols = pl.ds(pl.multiple_of(i * CHUNK, CHUNK), CHUNK)
            if j in WHOLE:
                value = weigh(pick[...], zr_a[j, :, :, :, cols].reshape(512, CHUNK))
            else:
                n = SPLIT.index(j)
                value = weigh(pick[:128, :], zr_s[n, :, :, :, cols].reshape(128, CHUNK))
                value = value + weigh(pick[128:224, :], zr_b[n, :, :, cols].reshape(96, CHUNK))
            if j == 0:
                acc[:, cols] = acc[:, cols] + value
            else:
                xbuf[j - 1, :, cols] = value.astype(BF16)

        if j != 0:
            xd[j] = remote(xbuf.at[j - 1], xr.at[j - 1], sxr.at[j], rxr.at[j], at_x(j))
            xd[j].start()

    for j in (1, 3):
        near[j].wait_recv()
        relay[j].start()
        tell[j].wait_recv()
        pack_split(j)
    experts(0)
    forward(1)
    forward(3)
    relay[1].wait_recv()
    relay[3].wait_recv()
    tell[2].wait_recv()
    pack_split(2)
    experts(1)
    forward(2)
    experts(3)
    combine(0)
    combine(1)
    experts(2)
    sum_over_y(3)
    combine(3)
    sum_over_y(2)
    combine(2)

    for j in (1, 3, 2):
        xd[j].wait_recv()
    y2 = {}
    for p in (1, 3, 2):
        cols = pl.ds(pl.multiple_of(lax.rem(y + p, 4) * 512, 512), 512)
        total = acc[:, cols]
        for j in range(3):
            total = total + xr[j, :, cols].astype(F32)
        y2s[p - 1] = total.astype(BF16)
        y2[p] = remote(y2s.at[p - 1], y2r.at[p - 1], sy2.at[p], ry2.at[p], at_y(p))
        y2[p].start()
    cols = pl.ds(pl.multiple_of(y * 512, 512), 512)
    total = acc[:, cols]
    for j in range(3):
        total = total + xr[j, :, cols].astype(F32)
    acc[:, cols] = total
    for p in (1, 3, 2):
        y2[p].wait_recv()
    total = acc[:, cols]
    for p in range(3):
        total = total + y2r[p].astype(F32)
    out[...] = total.astype(BF16)

    for group in (near, tell):
        for copy in group.values():
            copy.wait_send()
    for group in (zd, back, yb, xd, y2):
        for copy in group.values():
            copy.wait_send()


def layer(tokens, routes, gates, w_gate, w_up, w_down, s_gate, s_up, s_down):
    rows, width = tokens.shape
    ff, sff = w_gate.shape[2], s_gate.shape[1]
    routes_t = jnp.pad(routes.T, ((0, 2), (0, 0)), constant_values=-1)
    gates_t = jnp.pad(gates.T, ((0, 2), (0, 0)))
    vmem = pl.BlockSpec(memory_space=pltpu.VMEM)
    hbm = pl.BlockSpec(memory_space=pl.ANY)
    dma = pltpu.SemaphoreType.DMA
    return pl.pallas_call(
        kernel,
        out_shape=jax.ShapeDtypeStruct((rows, width // 4), BF16),
        in_specs=[vmem] * 3 + [hbm] * 6,
        out_specs=vmem,
        scratch_shapes=[
            pltpu.VMEM((16, rows), F32),
            pltpu.VMEM((3, 16, rows), F32),
            pltpu.VMEM((3, rows, width), BF16),
            pltpu.VMEM((4, 2, 8, 32, width), BF16),
            pltpu.VMEM((7, 2, 32, width), BF16),
            pltpu.VMEM((3, 2, 32, width), BF16),
            pltpu.VMEM((3, 6, 16, width), BF16),
            pltpu.VMEM((2, 3, 6, 16, width), BF16),
            pltpu.VMEM((2, 6, 16, width), BF16),
            pltpu.VMEM((2, 8, 2, 32, width), BF16),
            pltpu.VMEM((2, 2, 2, 32, width), BF16),
            pltpu.VMEM((2, 6, 16, width), BF16),
            pltpu.VMEM((3, rows, width), BF16),
            pltpu.VMEM((rows, width), F32),
            pltpu.VMEM((3, rows, width // 4), BF16),
            pltpu.VMEM((3, rows, width // 4), BF16),
            pltpu.VMEM((512, rows), BF16),
            pltpu.VMEM((256, ff), BF16),
            pltpu.VMEM((rows, sff), BF16),
            pltpu.VMEM(w_gate.shape, BF16),
            pltpu.VMEM(w_up.shape, BF16),
            pltpu.VMEM(w_down.shape, BF16),
            pltpu.VMEM(s_gate.shape, BF16),
            pltpu.VMEM(s_up.shape, BF16),
            pltpu.VMEM(s_down.shape, BF16),
            dma((4,)), dma((4,)),
            dma((3,)), dma((3,)),
            dma((4, 8)), dma((4, 8)),
            dma((4, 4)), dma((4, 4)),
            dma((4, 8)), dma((4, 8)),
            dma((4, 4)), dma((4, 4)),
            dma((4,)), dma((4,)),
            dma((4,)), dma((4,)),
            dma((6,)),
        ],
        compiler_params=pltpu.CompilerParams(
            collective_id=0, has_side_effects=True, vmem_limit_bytes=67043328
        ),
    )(tokens, routes_t, gates_t, w_gate, w_up, w_down, s_gate, s_up, s_down)


def solution(mesh):
    placed = (
        P("dp", None),
        P("dp", None),
        P("dp", None),
        P("dp", None, "expert"),
        P("dp", None, "expert"),
        P("dp", "expert", None),
        P(None, "expert"),
        P(None, "expert"),
        P("expert", None),
    )
    return jax.shard_map(
        layer, mesh=mesh, in_specs=placed, out_specs=P("dp", "expert"), check_vma=False
    )
```

```python
import jax
import jax.numpy as jnp
from jax import lax
from jax.experimental import pallas as pl
from jax.experimental.pallas import tpu as pltpu
from jax.sharding import PartitionSpec as P

MESH = pl.DeviceIdType.MESH
BF16 = jnp.bfloat16
F32 = jnp.float32
CAP = 32
CHUNK = 512
SENT = ((0, 1), (0, 1))
WHOLE = ((0, 1), (0, 3))
SPLIT = ((3, 2), (1, 2))
FAR = (2, 6, 4, 3, 7, 5)
SIDES = (0, 1)


def dot(a, b):
    return jnp.dot(a, b, preferred_element_type=F32)


def dot_t(a, b):
    return lax.dot_general(a, b, (((1,), (1,)), ((), ())), preferred_element_type=F32)


def silu(v):
    return v / (1.0 + jnp.exp(-v))


def kernel(
    tok, routes_t, gates_t, wg_h, wu_h, wd_h, sg_h, su_h, sd_h, out,
    info, xinfo, xbuf, slots, zst_a, zst_s, zst_b, ybuf_0, ybuf_1, ysum_0, ysum_1, zr_a, zr_s, zr_b, xr, acc, y2s, y2r,
    pick, weights, hid, shid, wg, wu, wd, sg, su, sd,
    sx, rx, si, ri, sz, rz, sy, ry, szr, rzr, syr, ryr, sxr, rxr, sy2, ry2, wsem,
):
    me = lax.axis_index("dp")
    y = lax.axis_index("expert")
    x = lax.div(me, 8)
    z = lax.rem(lax.div(me, 2), 4)
    c = lax.rem(me, 2)
    width = tok.shape[1]
    chunks = width // CHUNK
    side = width // 2
    strip = width // 8

    def core_of(cc):
        return c if cc == 0 else 1 - c

    def shifted(along_x, d, cc):
        if along_x:
            return lax.rem(x + d + 4, 4) * 8 + z * 2 + core_of(cc)
        return x * 8 + lax.rem(z + d + 4, 4) * 2 + core_of(cc)

    def gathered(s, d):
        return {"dp": shifted(s == 0, d, 0)}

    def across(s, d, cc):
        return {"dp": shifted(s == 1, d, cc)}

    def at_y(p):
        return {"expert": lax.rem(y + p, 4)}

    def remote(src, dst, s, r, where):
        return pltpu.make_async_remote_copy(
            src_ref=src, dst_ref=dst, send_sem=s, recv_sem=r, device_id=where, device_id_type=MESH
        )

    peers = [across(s, r // 2, r % 2) for s in SIDES for r in range(2, 8)]
    peers += [across(0, 0, 1)]
    peers += [at_y(p) for p in (1, 2, 3)]
    barrier = pltpu.get_barrier_semaphore()
    for peer in peers:
        pl.semaphore_signal(barrier, inc=1, device_id=peer, device_id_type=MESH)
    loads = [
        pltpu.make_async_copy(src, dst, wsem.at[i])
        for i, (src, dst) in enumerate(
            ((sg_h, sg), (su_h, su), (sd_h, sd), (wg_h, wg), (wu_h, wu), (wd_h, wd))
        )
    ]
    for load in loads:
        load.start()

    def half_of(s):
        return pl.ds(s * side, side)

    def piece(s, i):
        return pl.ds(pl.multiple_of(s * side + i * CHUNK, CHUNK), CHUNK)

    near, relay = {}, {}
    half = tok.shape[0] // 2
    for s in SIDES:
        cols = half_of(s)
        for n, (j, start) in enumerate(((1, 0), (3, half))):
            near[s, j] = remote(
                tok.at[:, cols], xbuf.at[j - 1, :, cols], sx.at[s, n], rx.at[s, n], gathered(s, -j)
            )
            relay[s, j] = remote(
                xbuf.at[j - 1, pl.ds(start, half), cols],
                xbuf.at[1, pl.ds(start, half), cols],
                sx.at[s, 2 + n],
                rx.at[s, 2 + n],
                gathered(s, -j),
            )
    rt = routes_t[...]
    rows = tok.shape[0]
    label = lax.broadcasted_iota(jnp.int32, (64, rows), 0)
    hits = jnp.zeros((64, rows), F32)
    for k in range(6):
        hits = hits + jnp.where(rt[k : k + 1, :] == label, 1.0, 0.0)
    earlier = jnp.where(
        lax.broadcasted_iota(jnp.int32, (rows, rows), 0)
        < lax.broadcasted_iota(jnp.int32, (rows, rows), 1),
        1.0,
        0.0,
    )
    before = dot(hits.astype(BF16), earlier.astype(BF16))
    info[...] = jnp.full(info.shape, -1.0, F32)
    for k in range(6):
        slot = jnp.sum(jnp.where(rt[k : k + 1, :] == label, before, 0.0), axis=0, keepdims=True)
        info[k : k + 1, :] = rt[k : k + 1, :].astype(F32) * CAP + slot
        info[8 + k : 9 + k, :] = gates_t[k : k + 1, :]
    tell = {}
    for j in (1, 3, 2):
        for s in SIDES:
            tell[s, j] = remote(
                info, xinfo.at[s * 3 + j - 1], si.at[s, j - 1], ri.at[s, j - 1], gathered(s, -j)
            )

    def base_of(s, r):
        return shifted(s == 1, r // 2, r % 2) * 64

    def place(s, j, r):
        if s == 0:
            return j, r
        return (4 - r // 2) % 4, 2 * ((4 - j) % 4) + r % 2

    def select(into, table, base, count, at, weighted):
        ids = (lax.broadcasted_iota(jnp.int32, (count, rows), 0) + base).astype(F32)
        value = jnp.zeros((count, rows), F32)
        for k in range(6):
            given = table[8 + k : 9 + k, :] if weighted else 1.0
            value = value + jnp.where(ids == table[k : k + 1, :], given, 0.0)
        into[at : at + count, :] = value.astype(BF16)

    def select_whole(into, table, s, weighted):
        for r in range(8):
            select(into, table, base_of(s, r), 64, r * 64, weighted)

    def select_split(into, table, s, weighted):
        for r in range(2):
            select(into, table, base_of(s, r), 64, r * 64, weighted)
        for r in range(2, 8):
            select(into, table, base_of(s, r) + 16 * y, 16, 128 + (r - 2) * 16, weighted)

    e_y, h_y = lax.div(y, 2), pl.multiple_of(lax.rem(y, 2) * 16, 16)

    zd = {}

    def pack(s, j):
        table = info if j == 0 else xinfo.at[s * 3 + j - 1]
        source = tok if j == 0 else xbuf.at[j - 1]
        mine, row = place(s, j, 0)
        split = j in SENT[s]
        if split:
            n = SENT[s].index(j)
            select_split(pick, table, s, False)
        else:
            n = 0 if j == 3 else 1
            select_whole(pick, table, s, False)

        @pl.loop(0, 2)
        def _(i):
            cols = piece(s, i)
            if split:
                packed = dot(pick[:224, :], source[:, cols]).astype(BF16)
                zst_s[n, :, :, cols] = packed[64:128].reshape(2, 32, CHUNK)
                zst_b[n, :, :, cols] = packed[128:224].reshape(6, 16, CHUNK)
            else:
                packed = dot(pick[...], source[:, cols]).astype(BF16)
                zst_a[n, :, :, :, cols] = packed[64:].reshape(7, 2, 32, CHUNK)
            slots[mine, :, row, :, cols] = packed[:64].reshape(2, 32, CHUNK)

    def send(s, j):
        table = info if j == 0 else xinfo.at[s * 3 + j - 1]
        split = j in SENT[s]
        n = SENT[s].index(j) if split else (0 if j == 3 else 1)
        cols = half_of(s)
        for r in FAR + (1,):
            block, to = place(s, j, r)
            whole = slots.at[block, :, to, :, cols]
            if not split:
                source, target = zst_a.at[n, r - 1, :, :, cols], whole
            elif r == 1:
                source, target = zst_s.at[n, :, :, cols], whole
            else:
                source = zst_b.at[n, r - 2, :, cols]
                target = slots.at[block, e_y, to, pl.ds(h_y, 16), cols]
            zd[s, j, r] = remote(
                source, target, sz.at[s, j, r - 1], rz.at[s, j, r - 1], across(s, r // 2, r % 2)
            )
            zd[s, j, r].start()
        if j in WHOLE[s]:
            select_whole(weights.at[s * 4 + j], table, s, True)
        else:
            select_split(weights.at[s * 4 + j], table, s, True)

    def shared():
        for load in loads[:3]:
            load.wait()
        gate = dot_t(tok[...], sg[...])
        up = dot_t(tok[...], su[...])
        shid[...] = (silu(gate) * up).astype(BF16)
        for h in SIDES:

            @pl.loop(0, 4)
            def _(i):
                given = pl.ds(pl.multiple_of(i * 2 * strip + h * strip, strip), strip)
                put = pl.ds(pl.multiple_of(h * side + i * strip, strip), strip)
                acc[:, put] = dot(shid[...], sd[:, given])

    yd = {}

    def forward(s, j):
        for r in FAR:
            zd[s, j, r].wait_recv()
        if s == 0:
            mine = slots.at[j, e_y, pl.ds(2, 6), pl.ds(h_y, 16), half_of(s)]
        else:
            row = place(s, j, 0)[1]
            mine = slots.at[pl.ds(1, 3), e_y, pl.ds(row, 2), pl.ds(h_y, 16), half_of(s)]
        for p in (1, 3, 2):
            yd[s, j, p] = remote(mine, mine, sy.at[s, j, p - 1], ry.at[s, j, p - 1], at_y(p))
            yd[s, j, p].start()

    back = {}
    yb = {}
    shared_on = set()

    def arrived(b):
        d = (4 - b) % 4
        if b in SENT[0]:
            sent = [(0, b)]
        else:
            sent = []
            for r in FAR:
                zd[0, b, r].wait_recv()
        zd[0, b, 1].wait_recv()
        for j in range(4):
            if d == 0:
                zd[1, j, 1].wait_recv()
            elif j in SENT[1]:
                sent.append((1, j))
            else:
                for r in (2 * d, 2 * d + 1):
                    zd[1, j, r].wait_recv()
        for s, j in sent:
            if (s, j) not in shared_on:
                shared_on.add((s, j))
                for p in (1, 3, 2):
                    yd[s, j, p].wait_recv()
                    yd[s, j, p].wait_send()

    def give_back(s, j, r, source, target):
        back[s, j, r] = remote(
            source, target, szr.at[s, j, r - 1], rzr.at[s, j, r - 1], across(s, -(r // 2), r % 2)
        )
        back[s, j, r].start()

    def give_to_y(s, b, rows_at, rows_n, target):
        for p in (1, 3, 2):
            to = lax.rem(y + p, 4)
            first = pl.multiple_of(lax.rem(to, 2) * 16, 16)
            yb[s, b, p] = remote(
                slots.at[b, lax.div(to, 2), pl.ds(rows_at, rows_n), pl.ds(first, 16), half_of(s)],
                target.at[p - 1],
                syr.at[s * 2 + b - 1 - (s == 0), p - 1],
                ryr.at[s * 2 + b - 1 - (s == 0), p - 1],
                at_y(p),
            )
            yb[s, b, p].start()

    def give_whole(b):
        n, cols = WHOLE[0].index(b), half_of(0)
        for r in FAR + (1,):
            give_back(0, b, r, slots.at[b, :, r, :, cols], zr_a.at[n, r, :, :, cols])

    def experts(b):
        arrived(b)

        @pl.loop(0, 2)
        def _(e):
            given = slots[b, e].reshape(256, width)
            gate = dot_t(given, wg[e])
            up = dot_t(given, wu[e])
            hid[e] = (silu(gate) * up).astype(BF16)

        for s in (1, 0):

            @pl.loop(0, 4)
            def _(i):
                given = pl.ds(pl.multiple_of(i * 2 * strip + s * strip, strip), strip)
                put = pl.ds(pl.multiple_of(s * side + i * strip, strip), strip)
                for e in range(2):
                    value = dot(hid[e], wd[e, :, given]).astype(BF16)
                    slots[b, e, :, :, put] = value.reshape(8, 32, strip)

            cols = half_of(s)
            d = (4 - b) % 4
            if s == 0:
                if b in WHOLE[0]:
                    n = WHOLE[0].index(b)
                    if b != 0:
                        give_whole(b)
                    zr_a[n, 0, :, :, cols] = slots[b, :, 0, :, cols]
                else:
                    n = SPLIT[0].index(b)
                    give_to_y(0, b, 2, 6, ybuf_0.at[n])
                    give_back(0, b, 1, slots.at[b, :, 1, :, cols], zr_s.at[n, 1, :, :, cols])
                    zr_s[n, 0, :, :, cols] = slots[b, :, 0, :, cols]
                continue
            if d != 0:
                give_to_y(1, b, 4, 4, ybuf_1.at[b - 1])
            for j in (3, 0, 1, 2):
                row = 2 * ((4 - j) % 4)
                if j in WHOLE[1]:
                    n, into = WHOLE[1].index(j), zr_a
                else:
                    n, into = SPLIT[1].index(j), zr_s
                if d == 0:
                    into[n, 0, :, :, cols] = slots[b, :, row, :, cols]
                    give_back(1, j, 1, slots.at[b, :, row + 1, :, cols], into.at[n, 1, :, :, cols])
                elif j in WHOLE[1]:
                    for cc in range(2):
                        give_back(
                            1,
                            j,
                            2 * d + cc,
                            slots.at[b, :, row + cc, :, cols],
                            zr_a.at[n, 2 * d + cc, :, :, cols],
                        )

    def sum_over_y(s, b):
        for p in (1, 3, 2):
            yb[s, b, p].wait_recv()
        if s == 0:
            n = SPLIT[0].index(b)
            rows_at, parts, into = 2, ybuf_0.at[n], ysum_0.at[n]
        else:
            rows_at, parts, into = 4, ybuf_1.at[b - 1], ysum_1.at[b - 1]
        for i in range(2):
            cols = pl.ds(i * CHUNK, CHUNK)
            total = slots[
                b, e_y, rows_at:8, pl.ds(h_y, 16), pl.ds(s * side + i * CHUNK, CHUNK)
            ].astype(F32)
            for p in range(3):
                total = total + parts[p, :, :, cols].astype(F32)
            into[:, :, cols] = total.astype(BF16)

        for row in range(rows_at, 8):
            if s == 0:
                j, r = b, row
            else:
                j, r = (4 - row // 2) % 4, 2 * ((4 - b) % 4) + row % 2
            give_back(
                s, j, r, into.at[row - rows_at], zr_b.at[SPLIT[s].index(j), r - 2, :, half_of(s)]
            )

    def weigh(a, b):
        return lax.dot_general(a, b, (((0,), (0,)), ((), ())), preferred_element_type=F32)

    xd = {}

    def combine(s, j):
        for r in range(1, 8):
            back[s, j, r].wait_recv()
        if (s, j) in relay:
            relay[s, j].wait_send()

        @pl.loop(0, 2)
        def _(i):
            cols = piece(s, i)
            if j in WHOLE[s]:
                n = WHOLE[s].index(j)
                value = weigh(weights[s * 4 + j], zr_a[n, :, :, :, cols].reshape(512, CHUNK))
            else:
                n = SPLIT[s].index(j)
                value = weigh(
                    weights[s * 4 + j, :128, :], zr_s[n, :, :, :, cols].reshape(128, CHUNK)
                )
                value = value + weigh(
                    weights[s * 4 + j, 128:224, :], zr_b[n, :, :, cols].reshape(96, CHUNK)
                )
            if j == 0:
                acc[:, cols] = acc[:, cols] + value
            else:
                xbuf[j - 1, :, cols] = value.astype(BF16)

        if j != 0:
            cols = half_of(s)
            xd[s, j] = remote(
                xbuf.at[j - 1, :, cols],
                xr.at[j - 1, :, cols],
                sxr.at[s, j - 1],
                rxr.at[s, j - 1],
                gathered(s, j),
            )
            xd[s, j].start()

    y2 = {}

    def finish(h):
        for j in (1, 3, 2):
            xd[h, j].wait_recv()
        part = pl.ds(h * strip, strip)
        for p in (1, 3, 2, 0):
            cols = pl.ds(pl.multiple_of(h * side + lax.rem(y + p, 4) * strip, strip), strip)
            total = acc[:, cols]
            for j in range(3):
                total = total + xr[j, :, cols].astype(F32)
            if p == 0:
                acc[:, cols] = total
                continue
            y2s[p - 1, :, part] = total.astype(BF16)
            y2[h, p] = remote(
                y2s.at[p - 1, :, part], y2r.at[p - 1, :, part], sy2.at[h, p - 1], ry2.at[h, p - 1], at_y(p)
            )
            y2[h, p].start()

    for s in SIDES:
        pack(s, 0)
    pl.semaphore_wait(barrier, len(peers))
    for j in (1, 3, 2):
        for s in SIDES:
            tell[s, j].start()
    for s in SIDES:
        send(s, 0)
    for j in (1, 3):
        for s in SIDES:
            near[s, j].start()
    shared()
    for s in SIDES:
        forward(s, 0)
    for j in (1, 3):
        for s in SIDES:
            near[s, j].wait_recv()
            relay[s, j].start()
        for s in SIDES:
            tell[s, j].wait_recv()
            pack(s, j)
            send(s, j)
    for s in SIDES:
        forward(s, 1)
    for load in loads[3:]:
        load.wait()
    for s in SIDES:
        relay[s, 1].wait_recv()
        relay[s, 3].wait_recv()
        tell[s, 2].wait_recv()
        pack(s, 2)
        send(s, 2)
    experts(0)
    experts(1)
    give_whole(0)
    experts(3)
    experts(2)
    sum_over_y(1, 1)
    sum_over_y(1, 3)
    sum_over_y(0, 3)
    sum_over_y(1, 2)
    combine(0, 1)
    combine(1, 3)
    combine(0, 3)
    combine(1, 1)
    sum_over_y(0, 2)
    combine(0, 0)
    combine(1, 0)
    combine(0, 2)
    combine(1, 2)
    finish(0)
    finish(1)
    def write_out(h):
        part = pl.ds(h * strip, strip)
        for p in (1, 3, 2):
            y2[h, p].wait_recv()
        total = acc[:, pl.ds(pl.multiple_of(h * side + y * strip, strip), strip)]
        for p in range(3):
            total = total + y2r[p, :, part].astype(F32)
        out[:, part] = total.astype(BF16)

    def drain():
        for group in (near, tell, zd, back, yb, xd, y2):
            for copy in group.values():
                copy.wait_send()

    write_out(0)
    write_out(1)
    drain()


def layer(tokens, routes, gates, w_gate, w_up, w_down, s_gate, s_up, s_down):
    rows, width = tokens.shape
    ff, sff = w_gate.shape[2], s_gate.shape[1]
    gate_t, up_t = jnp.swapaxes(w_gate, 1, 2), jnp.swapaxes(w_up, 1, 2)
    vmem = pl.BlockSpec(memory_space=pltpu.VMEM)
    hbm = pl.BlockSpec(memory_space=pl.ANY)
    dma = pltpu.SemaphoreType.DMA
    return pl.pallas_call(
        kernel,
        out_shape=jax.ShapeDtypeStruct((rows, width // 4), BF16),
        in_specs=[vmem] * 3 + [hbm] * 6,
        out_specs=vmem,
        scratch_shapes=[
            pltpu.VMEM((16, rows), F32),
            pltpu.VMEM((6, 16, rows), F32),
            pltpu.VMEM((3, rows, width), BF16),
            pltpu.VMEM((4, 2, 8, 32, width), BF16),
            pltpu.VMEM((2, 7, 2, 32, width), BF16),
            pltpu.VMEM((2, 2, 32, width), BF16),
            pltpu.VMEM((2, 6, 16, width), BF16),
            pltpu.VMEM((2, 3, 6, 16, width // 2), BF16),
            pltpu.VMEM((3, 3, 4, 16, width // 2), BF16),
            pltpu.VMEM((2, 6, 16, width // 2), BF16),
            pltpu.VMEM((3, 4, 16, width // 2), BF16),
            pltpu.VMEM((2, 8, 2, 32, width), BF16),
            pltpu.VMEM((2, 2, 2, 32, width), BF16),
            pltpu.VMEM((2, 6, 16, width), BF16),
            pltpu.VMEM((3, rows, width), BF16),
            pltpu.VMEM((rows, width), F32),
            pltpu.VMEM((3, rows, width // 4), BF16),
            pltpu.VMEM((3, rows, width // 4), BF16),
            pltpu.VMEM((512, rows), BF16),
            pltpu.VMEM((8, 512, rows), BF16),
            pltpu.VMEM((2, 256, ff), BF16),
            pltpu.VMEM((rows, sff), BF16),
            pltpu.VMEM(gate_t.shape, BF16),
            pltpu.VMEM(up_t.shape, BF16),
            pltpu.VMEM(w_down.shape, BF16),
            pltpu.VMEM((sff, width), BF16),
            pltpu.VMEM((sff, width), BF16),
            pltpu.VMEM(s_down.shape, BF16),
            dma((2, 4)), dma((2, 4)),
            dma((2, 3)), dma((2, 3)),
            dma((2, 4, 7)), dma((2, 4, 7)),
            dma((2, 2, 3)), dma((2, 2, 3)),
            dma((2, 4, 7)), dma((2, 4, 7)),
            dma((5, 3)), dma((5, 3)),
            dma((2, 3)), dma((2, 3)),
            dma((2, 3)), dma((2, 3)),
            dma((6,)),
        ],
        compiler_params=pltpu.CompilerParams(
            collective_id=0, has_side_effects=True, vmem_limit_bytes=67043328
        ),
    )(tokens, routes.T, gates.T, gate_t, up_t, w_down, s_gate.T, s_up.T, s_down)


def solution(mesh):
    placed = (
        P("dp", None),
        P("dp", None),
        P("dp", None),
        P("dp", None, "expert"),
        P("dp", None, "expert"),
        P("dp", "expert", None),
        P(None, "expert"),
        P(None, "expert"),
        P("expert", None),
    )
    return jax.shard_map(
        layer, mesh=mesh, in_specs=placed, out_specs=P("dp", "expert"), check_vma=False
    )
```

```python
import jax
import jax.numpy as jnp
from jax import lax
from jax.experimental import pallas as pl
from jax.experimental.pallas import tpu as pltpu
from jax.sharding import PartitionSpec as P

MESH = pl.DeviceIdType.MESH
BF16 = jnp.bfloat16
F32 = jnp.float32
CAP = 32
CHUNK = 512
SENT = ((0, 1), (0, 1))
WHOLE = ((0, 2), (0, 2))
SPLIT = ((1, 3), (1, 3))
FAR = (2, 6, 4, 3, 7, 5)
PAIRS = (2, 6)
SIDES = (0, 1)


def dot(a, b):
    return jnp.dot(a, b, preferred_element_type=F32)


def dot_t(a, b):
    return lax.dot_general(a, b, (((1,), (1,)), ((), ())), preferred_element_type=F32)


def silu(v):
    return v / (1.0 + jnp.exp(-v))


def kernel(
    tok, routes_t, gates_t, wg_h, wu_h, wd_h, sg_h, su_h, sd_h, out,
    info, xinfo, xbuf, slots, zst_a, zst_s, zst_b, ybuf_0, ybuf_1, ysum_0, ysum_1, zr_a, zr_s, zr_b, xr, acc, y2s, y2r,
    pick, weights, hid, shid, wg, wu, wd, sg, su, sd,
    sx, rx, si, ri, sz, rz, sy, ry, szr, rzr, syr, ryr, sxr, rxr, sy2, ry2, wsem,
):
    me = lax.axis_index("dp")
    y = lax.axis_index("expert")
    x = lax.div(me, 8)
    z = lax.rem(lax.div(me, 2), 4)
    c = lax.rem(me, 2)
    width = tok.shape[1]
    chunks = width // CHUNK
    side = width // 2
    strip = width // 8

    def core_of(cc):
        return c if cc == 0 else 1 - c

    def shifted(along_x, d, cc):
        if along_x:
            return lax.rem(x + d + 4, 4) * 8 + z * 2 + core_of(cc)
        return x * 8 + lax.rem(z + d + 4, 4) * 2 + core_of(cc)

    def gathered(s, d):
        return {"dp": shifted(s == 0, d, 0)}

    def across(s, d, cc):
        return {"dp": shifted(s == 1, d, cc)}

    def at_y(p):
        return {"expert": lax.rem(y + p, 4)}

    def remote(src, dst, s, r, where):
        return pltpu.make_async_remote_copy(
            src_ref=src, dst_ref=dst, send_sem=s, recv_sem=r, device_id=where, device_id_type=MESH
        )

    peers = [across(s, r // 2, r % 2) for s in SIDES for r in range(2, 8)]
    peers += [across(0, 0, 1)]
    peers += [at_y(p) for p in (1, 2, 3)]
    barrier = pltpu.get_barrier_semaphore()
    for peer in peers:
        pl.semaphore_signal(barrier, inc=1, device_id=peer, device_id_type=MESH)
    loads = [
        pltpu.make_async_copy(src, dst, wsem.at[i])
        for i, (src, dst) in enumerate(
            ((sg_h, sg), (su_h, su), (sd_h, sd), (wg_h, wg), (wu_h, wu), (wd_h, wd))
        )
    ]
    for load in loads:
        load.start()

    def half_of(s):
        return pl.ds(s * side, side)

    def piece(s, i):
        return pl.ds(pl.multiple_of(s * side + i * CHUNK, CHUNK), CHUNK)

    near, relay = {}, {}
    half = tok.shape[0] // 2
    for s in SIDES:
        cols = half_of(s)
        for n, (j, start) in enumerate(((1, 0), (3, half))):
            near[s, j] = remote(
                tok.at[:, cols], xbuf.at[j - 1, :, cols], sx.at[s, n], rx.at[s, n], gathered(s, -j)
            )
            relay[s, j] = remote(
                xbuf.at[j - 1, pl.ds(start, half), cols],
                xbuf.at[1, pl.ds(start, half), cols],
                sx.at[s, 2 + n],
                rx.at[s, 2 + n],
                gathered(s, -j),
            )
    rt = routes_t[...]
    rows = tok.shape[0]
    label = lax.broadcasted_iota(jnp.int32, (64, rows), 0)
    hits = jnp.zeros((64, rows), F32)
    for k in range(6):
        hits = hits + jnp.where(rt[k : k + 1, :] == label, 1.0, 0.0)
    earlier = jnp.where(
        lax.broadcasted_iota(jnp.int32, (rows, rows), 0)
        < lax.broadcasted_iota(jnp.int32, (rows, rows), 1),
        1.0,
        0.0,
    )
    before = dot(hits.astype(BF16), earlier.astype(BF16))
    info[...] = jnp.full(info.shape, -1.0, F32)
    for k in range(6):
        slot = jnp.sum(jnp.where(rt[k : k + 1, :] == label, before, 0.0), axis=0, keepdims=True)
        info[k : k + 1, :] = rt[k : k + 1, :].astype(F32) * CAP + slot
        info[8 + k : 9 + k, :] = gates_t[k : k + 1, :]
    tell = {}
    for j in (1, 3, 2):
        for s in SIDES:
            tell[s, j] = remote(
                info, xinfo.at[s * 3 + j - 1], si.at[s, j - 1], ri.at[s, j - 1], gathered(s, -j)
            )

    def base_of(s, r):
        return shifted(s == 1, r // 2, r % 2) * 64

    def place(s, j, r):
        if s == 0:
            return j, r
        return (4 - r // 2) % 4, 2 * ((4 - j) % 4) + r % 2

    def select(into, table, base, count, at, weighted):
        ids = (lax.broadcasted_iota(jnp.int32, (count, rows), 0) + base).astype(F32)
        value = jnp.zeros((count, rows), F32)
        for k in range(6):
            given = table[8 + k : 9 + k, :] if weighted else 1.0
            value = value + jnp.where(ids == table[k : k + 1, :], given, 0.0)
        into[at : at + count, :] = value.astype(BF16)

    def select_whole(into, table, s, weighted):
        for r in range(8):
            select(into, table, base_of(s, r), 64, r * 64, weighted)

    def select_split(into, table, s, weighted):
        for r in range(2):
            select(into, table, base_of(s, r), 64, r * 64, weighted)
        for r in range(2, 8):
            select(into, table, base_of(s, r) + 16 * y, 16, 128 + (r - 2) * 16, weighted)

    e_y, h_y = lax.div(y, 2), pl.multiple_of(lax.rem(y, 2) * 16, 16)

    zd = {}

    def pack(s, j):
        table = info if j == 0 else xinfo.at[s * 3 + j - 1]
        source = tok if j == 0 else xbuf.at[j - 1]
        mine, row = place(s, j, 0)
        split = j in SENT[s]
        if split:
            n = SENT[s].index(j)
            select_split(pick, table, s, False)
        else:
            n = 0 if j == 3 else 1
            select_whole(pick, table, s, False)

        @pl.loop(0, 2)
        def _(i):
            cols = piece(s, i)
            if split:
                packed = dot(pick[:224, :], source[:, cols]).astype(BF16)
                zst_s[n, :, :, cols] = packed[64:128].reshape(2, 32, CHUNK)
                zst_b[n, :, :, cols] = packed[128:224].reshape(6, 16, CHUNK)
            else:
                packed = dot(pick[...], source[:, cols]).astype(BF16)
                zst_a[n, :, :, :, cols] = packed[64:].reshape(7, 2, 32, CHUNK)
            slots[mine, :, row, :, cols] = packed[:64].reshape(2, 32, CHUNK)

    def send(s, j):
        table = info if j == 0 else xinfo.at[s * 3 + j - 1]
        split = j in SENT[s]
        n = SENT[s].index(j) if split else (0 if j == 3 else 1)
        cols = half_of(s)
        for r in FAR + (1,):
            block, to = place(s, j, r)
            whole = slots.at[block, :, to, :, cols]
            if not split:
                source, target = zst_a.at[n, r - 1, :, :, cols], whole
            elif r == 1:
                source, target = zst_s.at[n, :, :, cols], whole
            else:
                source = zst_b.at[n, r - 2, :, cols]
                target = slots.at[block, e_y, to, pl.ds(h_y, 16), cols]
            zd[s, j, r] = remote(
                source, target, sz.at[s, j, r - 1], rz.at[s, j, r - 1], across(s, r // 2, r % 2)
            )
            zd[s, j, r].start()
        if j in WHOLE[s]:
            select_whole(weights.at[s * 4 + j], table, s, True)
        else:
            select_split(weights.at[s * 4 + j], table, s, True)

    def shared():
        for load in loads[:3]:
            load.wait()
        gate = dot_t(tok[...], sg[...])
        up = dot_t(tok[...], su[...])
        shid[...] = (silu(gate) * up).astype(BF16)
        for h in SIDES:

            @pl.loop(0, 4)
            def _(i):
                given = pl.ds(pl.multiple_of(i * 2 * strip + h * strip, strip), strip)
                put = pl.ds(pl.multiple_of(h * side + i * strip, strip), strip)
                acc[:, put] = dot(shid[...], sd[:, given])

    yd = {}

    def forward(s, j):
        for r in FAR:
            zd[s, j, r].wait_recv()
        if s == 0:
            mine = slots.at[j, e_y, pl.ds(2, 6), pl.ds(h_y, 16), half_of(s)]
        else:
            row = place(s, j, 0)[1]
            mine = slots.at[pl.ds(1, 3), e_y, pl.ds(row, 2), pl.ds(h_y, 16), half_of(s)]
        for p in (1, 3, 2):
            yd[s, j, p] = remote(mine, mine, sy.at[s, j, p - 1], ry.at[s, j, p - 1], at_y(p))
            yd[s, j, p].start()

    back = {}
    yb = {}
    shared_on = set()

    def arrived(b):
        d = (4 - b) % 4
        if b in SENT[0]:
            sent = [(0, b)]
        else:
            sent = []
            for r in FAR:
                zd[0, b, r].wait_recv()
        zd[0, b, 1].wait_recv()
        for j in range(4):
            if d == 0:
                zd[1, j, 1].wait_recv()
            elif j in SENT[1]:
                sent.append((1, j))
            else:
                for r in (2 * d, 2 * d + 1):
                    zd[1, j, r].wait_recv()
        for s, j in sent:
            if (s, j) not in shared_on:
                shared_on.add((s, j))
                for p in (1, 3, 2):
                    yd[s, j, p].wait_recv()
                    yd[s, j, p].wait_send()

    def give_back(s, j, r, source, target):
        back[s, j, r] = remote(
            source, target, szr.at[s, j, r - 1], rzr.at[s, j, r - 1], across(s, -(r // 2), r % 2)
        )
        back[s, j, r].start()

    def give_to_y(s, b, part, rows_at, rows_n, target):
        which = b // 2 if s == 0 else 2 * b + part
        for p in (1, 3, 2):
            to = lax.rem(y + p, 4)
            first = pl.multiple_of(lax.rem(to, 2) * 16, 16)
            yb[s, b, part, p] = remote(
                slots.at[b, lax.div(to, 2), pl.ds(rows_at, rows_n), pl.ds(first, 16), half_of(s)],
                target.at[p - 1],
                syr.at[which, p - 1],
                ryr.at[which, p - 1],
                at_y(p),
            )
            yb[s, b, part, p].start()

    def give_whole(b):
        n, cols = WHOLE[0].index(b), half_of(0)
        for r in FAR + (1,):
            give_back(0, b, r, slots.at[b, :, r, :, cols], zr_a.at[n, r, :, :, cols])

    def experts(b):
        arrived(b)

        @pl.loop(0, 2)
        def _(e):
            given = slots[b, e].reshape(256, width)
            gate = dot_t(given, wg[e])
            up = dot_t(given, wu[e])
            hid[e] = (silu(gate) * up).astype(BF16)

        for s in (1, 0):

            @pl.loop(0, 4)
            def _(i):
                given = pl.ds(pl.multiple_of(i * 2 * strip + s * strip, strip), strip)
                put = pl.ds(pl.multiple_of(s * side + i * strip, strip), strip)
                for e in range(2):
                    value = dot(hid[e], wd[e, :, given]).astype(BF16)
                    slots[b, e, :, :, put] = value.reshape(8, 32, strip)

            cols = half_of(s)
            d = (4 - b) % 4
            if s == 0:
                if b in WHOLE[0]:
                    n = WHOLE[0].index(b)
                    give_whole(b)
                    zr_a[n, 0, :, :, cols] = slots[b, :, 0, :, cols]
                else:
                    n = SPLIT[0].index(b)
                    give_to_y(0, b, 0, 2, 6, ybuf_0.at[n])
                    give_back(0, b, 1, slots.at[b, :, 1, :, cols], zr_s.at[n, 1, :, :, cols])
                    zr_s[n, 0, :, :, cols] = slots[b, :, 0, :, cols]
                continue
            if d != 0:
                for part in range(2):
                    give_to_y(1, b, part, PAIRS[part], 2, ybuf_1.at[b - 1, part])
            for j in (2, 0, 1, 3):
                row = 2 * ((4 - j) % 4)
                if j in WHOLE[1]:
                    n, into = WHOLE[1].index(j), zr_a
                else:
                    n, into = SPLIT[1].index(j), zr_s
                if d == 0:
                    into[n, 0, :, :, cols] = slots[b, :, row, :, cols]
                    give_back(1, j, 1, slots.at[b, :, row + 1, :, cols], into.at[n, 1, :, :, cols])
                elif j in WHOLE[1]:
                    for cc in range(2):
                        give_back(
                            1,
                            j,
                            2 * d + cc,
                            slots.at[b, :, row + cc, :, cols],
                            zr_a.at[n, 2 * d + cc, :, :, cols],
                        )

    def sum_over_y(s, b):
        if s == 0:
            n = SPLIT[0].index(b)
            groups = ((0, 2, 6, ybuf_0.at[n], ysum_0.at[n]),)
        else:
            groups = tuple(
                (part, PAIRS[part], 2, ybuf_1.at[b - 1, part], ysum_1.at[b - 1, part])
                for part in range(2)
            )
        for part, rows_at, count, parts, into in groups:
            for p in (1, 3, 2):
                yb[s, b, part, p].wait_recv()
            for i in range(2):
                cols = pl.ds(i * CHUNK, CHUNK)
                total = slots[
                    b,
                    e_y,
                    rows_at : rows_at + count,
                    pl.ds(h_y, 16),
                    pl.ds(s * side + i * CHUNK, CHUNK),
                ].astype(F32)
                for p in range(3):
                    total = total + parts[p, :, :, cols].astype(F32)
                into[:, :, cols] = total.astype(BF16)
            for row in range(rows_at, rows_at + count):
                if s == 0:
                    j, r = b, row
                else:
                    j, r = (4 - row // 2) % 4, 2 * ((4 - b) % 4) + row % 2
                give_back(
                    s,
                    j,
                    r,
                    into.at[row - rows_at],
                    zr_b.at[SPLIT[s].index(j), r - 2, :, half_of(s)],
                )

    def weigh(a, b):
        return lax.dot_general(a, b, (((0,), (0,)), ((), ())), preferred_element_type=F32)

    xd = {}

    def combine(s, j):
        for r in range(1, 8):
            back[s, j, r].wait_recv()
        if (s, j) in relay:
            relay[s, j].wait_send()

        @pl.loop(0, 2)
        def _(i):
            cols = piece(s, i)
            if j in WHOLE[s]:
                n = WHOLE[s].index(j)
                value = weigh(weights[s * 4 + j], zr_a[n, :, :, :, cols].reshape(512, CHUNK))
            else:
                n = SPLIT[s].index(j)
                value = weigh(
                    weights[s * 4 + j, :128, :], zr_s[n, :, :, :, cols].reshape(128, CHUNK)
                )
                value = value + weigh(
                    weights[s * 4 + j, 128:224, :], zr_b[n, :, :, cols].reshape(96, CHUNK)
                )
            if j == 0:
                acc[:, cols] = acc[:, cols] + value
            else:
                xbuf[j - 1, :, cols] = value.astype(BF16)

        if j != 0:
            cols = half_of(s)
            xd[s, j] = remote(
                xbuf.at[j - 1, :, cols],
                xr.at[j - 1, :, cols],
                sxr.at[s, j - 1],
                rxr.at[s, j - 1],
                gathered(s, j),
            )
            xd[s, j].start()

    y2 = {}

    def finish(h):
        for j in (1, 3, 2):
            xd[h, j].wait_recv()
        part = pl.ds(h * strip, strip)
        for p in (1, 3, 2, 0):
            cols = pl.ds(pl.multiple_of(h * side + lax.rem(y + p, 4) * strip, strip), strip)
            total = acc[:, cols]
            for j in range(3):
                total = total + xr[j, :, cols].astype(F32)
            if p == 0:
                acc[:, cols] = total
                continue
            y2s[p - 1, :, part] = total.astype(BF16)
            y2[h, p] = remote(
                y2s.at[p - 1, :, part], y2r.at[p - 1, :, part], sy2.at[h, p - 1], ry2.at[h, p - 1], at_y(p)
            )
            y2[h, p].start()

    for s in SIDES:
        pack(s, 0)
    pl.semaphore_wait(barrier, len(peers))
    for j in (1, 3, 2):
        for s in SIDES:
            tell[s, j].start()
    for s in SIDES:
        send(s, 0)
    for j in (1, 3):
        for s in SIDES:
            near[s, j].start()
    shared()
    for s in SIDES:
        forward(s, 0)
    for j in (1, 3):
        for s in SIDES:
            near[s, j].wait_recv()
            relay[s, j].start()
        for s in SIDES:
            tell[s, j].wait_recv()
            pack(s, j)
            send(s, j)
    for s in SIDES:
        forward(s, 1)
    for load in loads[3:]:
        load.wait()
    for s in SIDES:
        relay[s, 1].wait_recv()
        relay[s, 3].wait_recv()
        tell[s, 2].wait_recv()
        pack(s, 2)
        send(s, 2)
    experts(0)
    experts(1)
    experts(2)
    experts(3)
    sum_over_y(1, 1)
    sum_over_y(0, 1)
    combine(0, 2)
    sum_over_y(1, 2)
    combine(1, 2)
    sum_over_y(1, 3)
    combine(0, 1)
    sum_over_y(0, 3)
    combine(0, 0)
    combine(1, 0)
    combine(0, 3)
    combine(1, 1)
    combine(1, 3)
    finish(0)
    finish(1)
    def write_out(h):
        part = pl.ds(h * strip, strip)
        for p in (1, 3, 2):
            y2[h, p].wait_recv()
        total = acc[:, pl.ds(pl.multiple_of(h * side + y * strip, strip), strip)]
        for p in range(3):
            total = total + y2r[p, :, part].astype(F32)
        out[:, part] = total.astype(BF16)

    def drain():
        for group in (near, tell, zd, back, yb, xd, y2):
            for copy in group.values():
                copy.wait_send()

    write_out(0)
    write_out(1)
    drain()


def layer(tokens, routes, gates, w_gate, w_up, w_down, s_gate, s_up, s_down):
    rows, width = tokens.shape
    ff, sff = w_gate.shape[2], s_gate.shape[1]
    gate_t, up_t = jnp.swapaxes(w_gate, 1, 2), jnp.swapaxes(w_up, 1, 2)
    vmem = pl.BlockSpec(memory_space=pltpu.VMEM)
    hbm = pl.BlockSpec(memory_space=pl.ANY)
    dma = pltpu.SemaphoreType.DMA
    return pl.pallas_call(
        kernel,
        out_shape=jax.ShapeDtypeStruct((rows, width // 4), BF16),
        in_specs=[vmem] * 3 + [hbm] * 6,
        out_specs=vmem,
        scratch_shapes=[
            pltpu.VMEM((16, rows), F32),
            pltpu.VMEM((6, 16, rows), F32),
            pltpu.VMEM((3, rows, width), BF16),
            pltpu.VMEM((4, 2, 8, 32, width), BF16),
            pltpu.VMEM((2, 7, 2, 32, width), BF16),
            pltpu.VMEM((2, 2, 32, width), BF16),
            pltpu.VMEM((2, 6, 16, width), BF16),
            pltpu.VMEM((2, 3, 6, 16, width // 2), BF16),
            pltpu.VMEM((3, 2, 3, 2, 16, width // 2), BF16),
            pltpu.VMEM((2, 6, 16, width // 2), BF16),
            pltpu.VMEM((3, 2, 2, 16, width // 2), BF16),
            pltpu.VMEM((2, 8, 2, 32, width), BF16),
            pltpu.VMEM((2, 2, 2, 32, width), BF16),
            pltpu.VMEM((2, 6, 16, width), BF16),
            pltpu.VMEM((3, rows, width), BF16),
            pltpu.VMEM((rows, width), F32),
            pltpu.VMEM((3, rows, width // 4), BF16),
            pltpu.VMEM((3, rows, width // 4), BF16),
            pltpu.VMEM((512, rows), BF16),
            pltpu.VMEM((8, 512, rows), BF16),
            pltpu.VMEM((2, 256, ff), BF16),
            pltpu.VMEM((rows, sff), BF16),
            pltpu.VMEM(gate_t.shape, BF16),
            pltpu.VMEM(up_t.shape, BF16),
            pltpu.VMEM(w_down.shape, BF16),
            pltpu.VMEM((sff, width), BF16),
            pltpu.VMEM((sff, width), BF16),
            pltpu.VMEM(s_down.shape, BF16),
            dma((2, 4)), dma((2, 4)),
            dma((2, 3)), dma((2, 3)),
            dma((2, 4, 7)), dma((2, 4, 7)),
            dma((2, 2, 3)), dma((2, 2, 3)),
            dma((2, 4, 7)), dma((2, 4, 7)),
            dma((8, 3)), dma((8, 3)),
            dma((2, 3)), dma((2, 3)),
            dma((2, 3)), dma((2, 3)),
            dma((6,)),
        ],
        compiler_params=pltpu.CompilerParams(
            collective_id=0, has_side_effects=True, vmem_limit_bytes=67043328
        ),
    )(tokens, routes.T, gates.T, gate_t, up_t, w_down, s_gate.T, s_up.T, s_down)


def solution(mesh):
    placed = (
        P("dp", None),
        P("dp", None),
        P("dp", None),
        P("dp", None, "expert"),
        P("dp", None, "expert"),
        P("dp", "expert", None),
        P(None, "expert"),
        P(None, "expert"),
        P("expert", None),
    )
    return jax.shard_map(
        layer, mesh=mesh, in_specs=placed, out_specs=P("dp", "expert"), check_vma=False
    )
```
